32 devices in a mesh: node: 32 (over z, y, x, core).
Axes of the slice: x: 2, y: 2, z: 4, core: 2. Of those that a mesh axis runs over, the one named last changes fastest.
Arguments:
- round_index: int32 [1], replicated, may hold values from 0 to 63
- sample_ids: int32 [32, 8], P('node'), may hold values from 0 to 3
- token_pool: bfloat16 [32, 4, 64, 512], P('node'), may hold values from -20 to 20
- cotangent_pool: bfloat16 [32, 4, 64, 512], P('node'), may hold values from -6 to 6
- weights: bfloat16 [32, 4, 512, 512], P('node'), may hold values from -12 to 12
- residue: bfloat16 [32, 4, 512, 512], P('node'), may hold values from -6 to 6
Outputs:
- new_weights: bfloat16 [32, 4, 512, 512], P('node')
- new_residue: bfloat16 [32, 4, 512, 512], P('node')
- grad_rms: float32 [], replicated
The draws below stay inside these ranges and needn't reach their ends.
All inputs are finite; a program needn't handle non-finite values.
Results may differ from the reference program's by a relative error of at most 0.0065.
Values may be sent and summed in bfloat16 or wider, within the bound.
A program may use at most 128 MiB of HBM per device.

```python
import jax
import jax.numpy as jnp
from jax import lax

HEAD_DIM = 64
D = 512
SEQ = 64
BATCH = 8
POOL = 4
NODES = 32
N_NODE = 32


def draw_weights(key, part):
    shape_all = (NODES, 4, D, D)
    drawn = jax.random.normal(key, shape_all, jnp.float32)
    return jnp.clip(drawn, -12.0, 12.0).astype(jnp.bfloat16)


def draw_token_pool(key, part):
    shape_all = (NODES, POOL, SEQ, D)
    drawn = jax.random.normal(key, shape_all, jnp.float32)
    return jnp.clip(drawn, -20.0, 20.0).astype(jnp.bfloat16)


def draw_cotangent_pool(key, part):
    shape_all = (NODES, POOL, SEQ, D)
    rising = (jnp.arange(NODES, dtype=jnp.float32) / max(NODES - 1, 1)).reshape(NODES, 1, 1, 1)
    drawn = jax.random.normal(key, shape_all, jnp.float32) * 0.5 * jnp.power(3.0, 0.5 * rising)
    return jnp.clip(drawn, -6.0, 6.0).astype(jnp.bfloat16)


def place_ends(values, stream_key, smallest, high):
    longest = values.shape.index(max(values.shape))
    spots = []
    for shift in (0, 1):
        where = [jax.random.randint(jax.random.fold_in(stream_key, axis), (), 0, length) for axis, length in enumerate(values.shape)]
        where[longest] = (where[longest] + shift) % values.shape[longest]
        spots.append(tuple(where))
    return values.at[spots[0]].set(smallest).at[spots[1]].set(high)


def steps_of(stream_key, extent, cuts, smallest, top_value):
    gain, own = 1.0, jax.random.fold_in(stream_key, 6)
    for axis_at, parts in cuts:
        heights = jnp.exp(jax.random.uniform(jax.random.fold_in(own, axis_at), (parts,), jnp.float32, smallest / len(cuts), top_value / len(cuts)))
        gain = gain * jnp.repeat(heights, extent[axis_at] // parts).reshape([-1 if axis == axis_at else 1 for axis in range(len(extent))])
    return gain


def centred(own_key, dims, scale, most, shards=(), held_as=jnp.bfloat16):
    entries = jax.random.normal(own_key, dims, jnp.float32) * scale
    if len(shards) > 0:
        entries = steps_of(own_key, dims, shards, -0.22, 0.18) * entries
    return jnp.clip(entries, min=-most, max=most).astype(held_as)


def setup_inputs(seed: int = 0) -> dict:
    keys = jax.random.split(jax.random.key(seed), 7)
    round_index = jax.random.randint(keys[0], (1,), 0, 64).astype(jnp.int32)
    sample_ids = place_ends(jax.random.randint(keys[1], (NODES, BATCH), 0, POOL), jax.random.fold_in(keys[1], 1), 0, POOL - 1).astype(jnp.int32)
    token_pool = draw_token_pool(jax.random.fold_in(keys[6], 71), 0)
    cotangent_pool = draw_cotangent_pool(jax.random.fold_in(keys[6], 71), 0)
    weights = draw_weights(jax.random.fold_in(keys[6], 71), 0)
    residue = centred(keys[5], (NODES, 4, D, D), 1.0, 6.0, ((0, 32),))
    return {"round_index": round_index, "sample_ids": sample_ids, "token_pool": token_pool, "cotangent_pool": cotangent_pool, "weights": weights, "residue": residue}


epsilon = 1e-06
step_rate = 0.1

def normalize(tokens):
    values = tokens.astype(jnp.float32)
    centered = values - lax.optimization_barrier(jnp.mean(values, -1, keepdims=True))
    variance = lax.optimization_barrier(jnp.mean(centered * centered, -1, keepdims=True))
    return (centered * lax.rsqrt(variance + epsilon)).astype(jnp.bfloat16)

def node_gradient(weights, tokens, cotangent):
    batch_size, seq_len, model_width = tokens.shape
    head_count = model_width // HEAD_DIM
    proj_scale = model_width ** (-0.5)
    head_scale = HEAD_DIM ** (-0.5)
    row_count = batch_size * seq_len
    normed_rows = normalize(tokens).reshape(row_count, model_width)
    grad_rows = cotangent.reshape(row_count, model_width)

    def project(which):
        return (jnp.dot(normed_rows, weights[which], preferred_element_type=jnp.float32) * proj_scale).astype(jnp.bfloat16)

    def to_heads(matrix):
        return matrix.reshape(batch_size, seq_len, head_count, HEAD_DIM).astype(jnp.float32)
    queries = to_heads(project(0))
    key_rows = to_heads(project(1))
    value_rows = to_heads(project(2))
    scores = jnp.einsum('bshe,bthe->bhst', queries, key_rows) * head_scale
    attn_probs = jnp.exp(scores - lax.optimization_barrier(jnp.max(scores, -1, keepdims=True)))
    attn_probs = attn_probs / lax.optimization_barrier(jnp.sum(attn_probs, -1, keepdims=True))
    probs_half = attn_probs.astype(jnp.bfloat16).astype(jnp.float32)
    context = jnp.einsum('bhst,bthe->bshe', probs_half, value_rows).astype(jnp.bfloat16).reshape(row_count, model_width)
    grad_out = jnp.dot(context.T, grad_rows, preferred_element_type=jnp.float32) * proj_scale
    context_grad = (jnp.dot(grad_rows, weights[3].T, preferred_element_type=jnp.float32) * proj_scale).astype(jnp.bfloat16)
    context_heads = to_heads(context_grad)
    probs_grad = jnp.einsum('bshe,bthe->bhst', context_heads, value_rows)
    value_grad = jnp.einsum('bhst,bshe->bthe', probs_half, context_heads).astype(jnp.bfloat16)
    score_grad = (attn_probs * (probs_grad - lax.optimization_barrier(jnp.sum(probs_grad * attn_probs, -1, keepdims=True))) * head_scale).astype(jnp.bfloat16).astype(jnp.float32)
    query_grad = jnp.einsum('bhst,bthe->bshe', score_grad, key_rows).astype(jnp.bfloat16)
    key_grad = jnp.einsum('bhst,bshe->bthe', score_grad, queries).astype(jnp.bfloat16)

    def weight_grad(rows_grad):
        return jnp.dot(normed_rows.T, rows_grad.reshape(row_count, model_width), preferred_element_type=jnp.float32) * proj_scale
    return jnp.stack([weight_grad(query_grad), weight_grad(key_grad), weight_grad(value_grad), grad_out])

def reference(round_index, sample_ids, token_pool, cotangent_pool, weights, residue):

    def per_node(node_index):
        sample_rows = sample_ids[node_index]
        tokens = jnp.take(token_pool[node_index], sample_rows, axis=0)
        cotangent = jnp.take(cotangent_pool[node_index], sample_rows, axis=0)
        gradient = node_gradient(weights[node_index], tokens, cotangent)
        tracked = (residue[node_index].astype(jnp.float32) + gradient).astype(jnp.bfloat16)
        return (tracked, gradient, jnp.sum(gradient * gradient))
    tracked, gradient, squares = lax.map(per_node, jnp.arange(N_NODE, dtype=jnp.int32))
    levels = N_NODE.bit_length() - 1
    offset = jnp.left_shift(jnp.int32(1), round_index[0] % levels)

    def track_node(node_index):
        peer_index = (node_index - offset) % N_NODE
        tracker = 0.5 * (tracked[node_index].astype(jnp.float32) + tracked[peer_index].astype(jnp.float32))
        sent = (weights[node_index].astype(jnp.float32) - step_rate * tracker).astype(jnp.bfloat16)
        return (tracker, sent)
    tracker_all, sent_all = lax.map(track_node, jnp.arange(N_NODE, dtype=jnp.int32))

    def mix_node(node_index):
        peer_index = (node_index - offset) % N_NODE
        tracker = tracker_all[node_index]
        mixed = 0.5 * weights[node_index].astype(jnp.float32) + 0.5 * sent_all[peer_index].astype(jnp.float32) - 0.5 * step_rate * tracker
        return (mixed.astype(jnp.bfloat16), (tracker - gradient[node_index]).astype(jnp.bfloat16))
    new_weights, new_residue = lax.map(mix_node, jnp.arange(N_NODE, dtype=jnp.int32))
    grad_rms = jnp.sqrt(jnp.sum(squares) / (N_NODE * gradient[0].size))
    return (new_weights, new_residue, grad_rms)
```

```python
from functools import partial

import jax
import jax.numpy as jnp
from jax import lax
from jax.experimental import pallas as pl
from jax.experimental.pallas import tpu as pltpu
from jax.sharding import PartitionSpec as P

HEAD_DIM = 64
LANES = 128
CHUNK_ROWS = 128

epsilon = 1e-06
step_rate = 0.1

f32, bf16 = jnp.float32, jnp.bfloat16
MESH = pl.DeviceIdType.MESH
VMEM = pl.BlockSpec(memory_space=pltpu.VMEM)
SMEM = pl.BlockSpec(memory_space=pltpu.SMEM)
HBM = pl.BlockSpec(memory_space=pl.ANY)


def dot(left, right, left_dim=1, right_dim=0):
    return lax.dot_general(
        left, right, (((left_dim,), (right_dim,)), ((), ())), preferred_element_type=f32
    )


def factors_kernel(ids_ref, tokens_ref, cot_ref, weights_ref, left_ref, right_ref, context_ref):
    pool, seq, width = tokens_ref.shape[1:]
    batch = ids_ref.shape[1]
    rows = pool * seq
    proj_scale = width**-0.5
    head_scale = HEAD_DIM**-0.5
    pairs = width // LANES

    counts = []
    for image in range(pool):
        count = jnp.int32(0)
        for draw in range(batch):
            count = count + (ids_ref[0, draw] == image).astype(jnp.int32)
        counts.append(count.astype(f32))

    values = tokens_ref[0].reshape(rows, width).astype(f32)
    cot = cot_ref[0].reshape(rows, width)
    centered = values - jnp.mean(values, -1, keepdims=True)
    variance = jnp.mean(centered * centered, -1, keepdims=True)
    unit_rows = centered * lax.rsqrt(variance + epsilon)
    normed = unit_rows.astype(bf16)

    weighted = jnp.concatenate(
        [unit_rows[i * seq : (i + 1) * seq] * counts[i] for i in range(pool)], 0
    )
    left_ref[0] = weighted.T.astype(bf16)

    queries, keys, vals = [
        (dot(normed, weights_ref[0, m]) * proj_scale).astype(bf16) for m in range(3)
    ]
    context_grad = (dot(cot, weights_ref[0, 3], 1, 1) * proj_scale).astype(bf16)
    right_ref[3] = cot

    first = lax.broadcasted_iota(jnp.int32, (seq, LANES), 1) < HEAD_DIM
    units = [(i, j) for i in range(pool) for j in range(pairs)]

    def cut(matrix, unit):
        i, j = unit
        return matrix[i * seq : (i + 1) * seq, j * LANES : (j + 1) * LANES]

    def spread(block):
        zero = jnp.zeros_like(block)
        return jnp.concatenate([jnp.where(first, block, zero), jnp.where(first, zero, block)], 0)

    def gather(block):
        return jnp.where(first, block[:seq], block[seq:])

    queries2 = [spread(cut(queries, u)) for u in units]
    grads2 = [spread(cut(context_grad, u)) for u in units]
    keys1 = [cut(keys, u) for u in units]
    vals1 = [cut(vals, u) for u in units]

    scores = [dot(q, k, 1, 1) * head_scale for q, k in zip(queries2, keys1)]
    probs_grad = [dot(g, v, 1, 1) for g, v in zip(grads2, vals1)]
    probs, score_grad = [], []
    for s in scores:
        e = jnp.exp(s - jnp.max(s, -1, keepdims=True))
        probs.append(e / jnp.sum(e, -1, keepdims=True))
    half = [p.astype(bf16) for p in probs]
    for p, g in zip(probs, probs_grad):
        inner = jnp.sum(g * p, -1, keepdims=True)
        score_grad.append((p * (g - inner) * head_scale).astype(bf16))
    for n, (i, j) in enumerate(units):
        at = (slice(i * seq, (i + 1) * seq), slice(j * LANES, (j + 1) * LANES))
        context_ref[at] = gather(dot(half[n], vals1[n])) * counts[i]
        right_ref[2, at[0], at[1]] = dot(half[n], grads2[n], 0, 0).astype(bf16)
        right_ref[0, at[0], at[1]] = gather(dot(score_grad[n], keys1[n])).astype(bf16)
        right_ref[1, at[0], at[1]] = dot(score_grad[n], queries2[n], 0, 0).astype(bf16)
    left_ref[1] = context_ref[...].T.astype(bf16)


def exchange_kernel(
    nodes,
    offset,
    left_ref,
    right_ref,
    weights_ref,
    residue_ref,
    new_weights_ref,
    new_residue_ref,
    total_ref,
    gradient,
    tracked,
    tracked_in,
    sent,
    sent_in,
    weights_out,
    residue_out,
    squares,
    squares_in,
    track_send,
    track_recv,
    sent_send,
    sent_recv,
    out_sems,
    sum_send,
    sum_recv,
):
    me = lax.axis_index("node")
    target = lax.rem(me + offset, nodes)
    source = lax.rem(me + nodes - offset, nodes)
    steps = nodes.bit_length() - 1
    strides = [offset] + [2**k for k in range(steps) if 2**k != offset]
    partners = [me + stride * (1 - 2 * ((me // stride) % 2)) for stride in strides]
    matrices, width = weights_ref.shape[1], weights_ref.shape[2]
    per_matrix = width // CHUNK_ROWS
    chunks = matrices * per_matrix
    proj_scale = width**-0.5

    barrier = pltpu.get_barrier_semaphore()
    for other in [target, source] + partners:
        pl.semaphore_signal(barrier, inc=1, device_id=(other,), device_id_type=MESH)
    pl.semaphore_wait(barrier, 2 + steps)

    def place(c):
        return c // per_matrix, pl.ds((c % per_matrix) * CHUNK_ROWS, CHUNK_ROWS)

    def track_copy(c):
        return pltpu.make_async_remote_copy(
            tracked.at[c], tracked_in.at[c], track_send.at[c], track_recv.at[c], (target,), MESH
        )

    def sent_copy(c):
        return pltpu.make_async_remote_copy(
            sent.at[c], sent_in.at[c], sent_send.at[c], sent_recv.at[c], (target,), MESH
        )

    def residue_copy(c):
        m, rows = place(c)
        return pltpu.make_async_copy(
            residue_out.at[c], new_residue_ref.at[0, m, rows], out_sems.at[0, c]
        )

    def weights_copy(c):
        m, rows = place(c)
        return pltpu.make_async_copy(
            weights_out.at[c], new_weights_ref.at[0, m, rows], out_sems.at[1, c]
        )

    squares[...] = jnp.zeros_like(squares)

    @pl.loop(0, chunks)
    def _(c):
        m, rows = place(c)
        grad = dot(left_ref[m // 3, rows], right_ref[m]) * proj_scale
        gradient[c] = grad
        tracked[c] = (residue_ref[0, m, rows].astype(f32) + grad).astype(bf16)
        track_copy(c).start()
        squares[0] += jnp.sum((grad * grad).reshape(-1, 8, width), 0)

    folded = squares[0]
    squares[0, :, 0:LANES] = sum(
        folded[:, i * LANES : (i + 1) * LANES] for i in range(width // LANES)
    )

    def sum_copy(k):
        return pltpu.make_async_remote_copy(
            squares.at[k, :, pl.ds(0, LANES)],
            squares_in.at[k],
            sum_send.at[k],
            sum_recv.at[k],
            (partners[k],),
            MESH,
        )

    def sum_finish(k):
        sum_copy(k).wait()
        squares[k + 1, :, 0:LANES] = squares[k, :, 0:LANES] + squares_in[k]

    sum_copy(0).start()

    @pl.loop(0, chunks)
    def _(c):
        m, rows = place(c)
        track_copy(c).wait_recv()
        tracker = 0.5 * (tracked[c].astype(f32) + tracked_in[c].astype(f32))
        own = weights_ref[0, m, rows].astype(f32)
        sent[c] = (own - step_rate * tracker).astype(bf16)
        sent_copy(c).start()
        residue_out[c] = (tracker - gradient[c]).astype(bf16)
        residue_copy(c).start()
        gradient[c] = 0.5 * own - 0.5 * step_rate * tracker

    sum_finish(0)
    cuts = [(chunks * k) // steps for k in range(steps + 1)]
    for k in range(steps):
        if k >= 1:
            sum_copy(k).start()

        @pl.loop(cuts[k], cuts[k + 1])
        def _(c):
            sent_copy(c).wait_recv()
            weights_out[c] = (gradient[c] + 0.5 * sent_in[c].astype(f32)).astype(bf16)
            weights_copy(c).start()

        if k >= 1:
            sum_finish(k)
    total_ref[...] = squares[steps, :, 0:LANES]

    @pl.loop(0, chunks)
    def _(c):
        track_copy(c).wait_send()
        sent_copy(c).wait_send()
        residue_copy(c).wait()
        weights_copy(c).wait()


def exchange(nodes, level, left, right, weights, residue):
    matrices, width = weights.shape[1], weights.shape[2]
    chunks = matrices * (width // CHUNK_ROWS)
    steps = nodes.bit_length() - 1
    chunked = (chunks, CHUNK_ROWS, width)
    return pl.pallas_call(
        partial(exchange_kernel, nodes, 2**level),
        out_shape=(
            jax.ShapeDtypeStruct(weights.shape, bf16),
            jax.ShapeDtypeStruct(weights.shape, bf16),
            jax.ShapeDtypeStruct((8, LANES), f32),
        ),
        in_specs=[VMEM] * 4,
        out_specs=(HBM, HBM, VMEM),
        scratch_shapes=[
            pltpu.VMEM(chunked, f32),
            pltpu.VMEM(chunked, bf16),
            pltpu.VMEM(chunked, bf16),
            pltpu.VMEM(chunked, bf16),
            pltpu.VMEM(chunked, bf16),
            pltpu.VMEM(chunked, bf16),
            pltpu.VMEM(chunked, bf16),
            pltpu.VMEM((steps + 1, 8, width), f32),
            pltpu.VMEM((steps, 8, LANES), f32),
            pltpu.SemaphoreType.DMA((chunks,)),
            pltpu.SemaphoreType.DMA((chunks,)),
            pltpu.SemaphoreType.DMA((chunks,)),
            pltpu.SemaphoreType.DMA((chunks,)),
            pltpu.SemaphoreType.DMA((2, chunks)),
            pltpu.SemaphoreType.DMA((steps,)),
            pltpu.SemaphoreType.DMA((steps,)),
        ],
        compiler_params=pltpu.CompilerParams(collective_id=level, has_side_effects=True),
    )(left, right, weights, residue)


def per_device(round_index, sample_ids, token_pool, cotangent_pool, weights, residue):
    nodes = lax.axis_size("node")
    levels = nodes.bit_length() - 1
    pool, seq, width = token_pool.shape[1:]
    rows = pool * seq
    left, right = pl.pallas_call(
        factors_kernel,
        out_shape=(
            jax.ShapeDtypeStruct((2, width, rows), bf16),
            jax.ShapeDtypeStruct((4, rows, width), bf16),
        ),
        in_specs=[SMEM, VMEM, VMEM, VMEM],
        out_specs=(VMEM, VMEM),
        scratch_shapes=[pltpu.VMEM((rows, width), f32)],
    )(sample_ids, token_pool, cotangent_pool, weights)
    new_weights, new_residue, squares = lax.switch(
        round_index[0] % levels,
        [partial(exchange, nodes, level) for level in range(levels)],
        left,
        right,
        weights,
        residue,
    )
    grad_rms = jnp.sqrt(jnp.sum(squares) / (nodes * weights.size))
    return (new_weights, new_residue, grad_rms)


def solution(mesh):
    placed = (
        P(),
        P("node", None),
        P("node", None, None, None),
        P("node", None, None, None),
        P("node", None, None, None),
        P("node", None, None, None),
    )
    return jax.shard_map(
        per_device,
        mesh=mesh,
        in_specs=placed,
        out_specs=(P("node", None, None, None), P("node", None, None, None), P()),
        check_vma=False,
    )
```

```python
from functools import partial

import jax
import jax.numpy as jnp
from jax import lax
from jax.experimental import pallas as pl
from jax.experimental.pallas import tpu as pltpu
from jax.sharding import PartitionSpec as P

HEAD_DIM = 64
LANES = 128
CHUNK_ROWS = 128

epsilon = 1e-06
step_rate = 0.1

f32, bf16 = jnp.float32, jnp.bfloat16
MESH = pl.DeviceIdType.MESH
VMEM = pl.BlockSpec(memory_space=pltpu.VMEM)
SMEM = pl.BlockSpec(memory_space=pltpu.SMEM)
HBM = pl.BlockSpec(memory_space=pl.ANY)


def dot(left, right, left_dim=1, right_dim=0):
    return lax.dot_general(
        left, right, (((left_dim,), (right_dim,)), ((), ())), preferred_element_type=f32
    )


def round_kernel(
    nodes,
    offset,
    ids_ref,
    tokens_hbm,
    cot_hbm,
    weights_hbm,
    residue_hbm,
    new_weights_ref,
    new_residue_ref,
    rms_ref,
    tokens_ref,
    cot_ref,
    weights_ref,
    residue_ref,
    left_ref,
    right_ref,
    context_ref,
    gradient,
    tracked,
    tracked_in,
    sent,
    sent_in,
    squares,
    totals,
    totals_in,
    load_sems,
    track_send,
    track_recv,
    sent_send,
    sent_recv,
    sum_send,
    sum_recv,
):
    me = lax.axis_index("node")
    target = lax.rem(me + offset, nodes)
    source = lax.rem(me + nodes - offset, nodes)
    steps = nodes.bit_length() - 1
    strides = [offset] + [2**k for k in range(steps) if 2**k != offset]
    partners = [me + stride * (1 - 2 * ((me // stride) % 2)) for stride in strides]

    barrier = pltpu.get_barrier_semaphore()
    for other in [target, source] + partners:
        pl.semaphore_signal(barrier, inc=1, device_id=(other,), device_id_type=MESH)

    pool, seq, width = tokens_ref.shape
    matrices = weights_ref.shape[0]
    batch = ids_ref.shape[1]
    rows = pool * seq
    pairs = width // LANES
    per_matrix = width // CHUNK_ROWS
    proj_scale = width**-0.5
    head_scale = HEAD_DIM**-0.5
    order = [3, 2, 0, 1]

    moves = {"tokens": (tokens_hbm.at[0], tokens_ref), "cot": (cot_hbm.at[0], cot_ref)}
    for m in range(matrices):
        moves["w", m] = (weights_hbm.at[0, m], weights_ref.at[m])
        moves["r", m] = (residue_hbm.at[0, m], residue_ref.at[m])
    when = ["tokens", ("w", 0), ("w", 1), ("w", 2), "cot", ("r", 3), ("w", 3), ("r", 2), ("r", 0), ("r", 1)]
    loads = {name: pltpu.make_async_copy(*moves[name], load_sems.at[n]) for n, name in enumerate(when)}
    for name in when:
        loads[name].start()

    counts = []
    for image in range(pool):
        count = jnp.int32(0)
        for draw in range(batch):
            count = count + (ids_ref[0, draw] == image).astype(jnp.int32)
        counts.append(count.astype(f32))

    loads["tokens"].wait()
    values = tokens_ref[...].reshape(rows, width).astype(f32)
    centered = values - jnp.mean(values, -1, keepdims=True)
    variance = jnp.mean(centered * centered, -1, keepdims=True)
    unit_rows = centered * lax.rsqrt(variance + epsilon)
    normed = unit_rows.astype(bf16)
    projected = []
    for m in range(3):
        loads["w", m].wait()
        projected.append((dot(normed, weights_ref[m]) * proj_scale).astype(bf16))
    queries, keys, vals = projected

    first = lax.broadcasted_iota(jnp.int32, (seq, LANES), 1) < HEAD_DIM
    units = [(i, j) for i in range(pool) for j in range(pairs)]
    spots = [
        (slice(i * seq, (i + 1) * seq), slice(j * LANES, (j + 1) * LANES)) for i, j in units
    ]

    def spread(block):
        zero = jnp.zeros_like(block)
        return jnp.concatenate([jnp.where(first, block, zero), jnp.where(first, zero, block)], 0)

    def gather(block):
        return jnp.where(first, block[:seq], block[seq:])

    queries2 = [spread(queries[at]) for at in spots]
    keys1 = [keys[at] for at in spots]
    vals1 = [vals[at] for at in spots]
    scores = [dot(q, k, 1, 1) * head_scale for q, k in zip(queries2, keys1)]
    probs = []
    for s in scores:
        e = jnp.exp(s - jnp.max(s, -1, keepdims=True))
        probs.append(e / jnp.sum(e, -1, keepdims=True))
    half = [p.astype(bf16) for p in probs]
    for n, at in enumerate(spots):
        context_ref[at] = gather(dot(half[n], vals1[n])) * counts[units[n][0]]
    left_ref[1] = context_ref[...].T.astype(bf16)

    def track_copy(c):
        return pltpu.make_async_remote_copy(
            tracked.at[c], tracked_in.at[c], track_send.at[c], track_recv.at[c], (target,), MESH
        )

    def sent_copy(c):
        return pltpu.make_async_remote_copy(
            sent.at[c], sent_in.at[c], sent_send.at[c], sent_recv.at[c], (target,), MESH
        )

    def each_block(which, body):
        for m in which:

            @pl.loop(0, per_matrix)
            def _(r):
                body(m, pl.ds(r * CHUNK_ROWS, CHUNK_ROWS), order.index(m) * per_matrix + r)

    def track(m, part, c):
        right = right_ref[m] if m < 3 else cot_ref[...].reshape(rows, width)
        grad = dot(left_ref[m // 3, part], right) * proj_scale
        gradient[c] = grad
        tracked[c] = (residue_ref[m, part].astype(f32) + grad).astype(bf16)
        track_copy(c).start()
        squares[...] += jnp.sum((grad * grad).reshape(-1, 8, width), 0)

    squares[...] = jnp.zeros_like(squares)
    loads["cot"].wait()
    loads["r", 3].wait()
    pl.semaphore_wait(barrier, 2 + steps)
    each_block([3], track)

    loads["w", 3].wait()
    cot = cot_ref[...].reshape(rows, width)
    context_grad = (dot(cot, weights_ref[3], 1, 1) * proj_scale).astype(bf16)
    weighted = [unit_rows[i * seq : (i + 1) * seq] * counts[i] for i in range(pool)]
    left_ref[0] = jnp.concatenate(weighted, 0).T.astype(bf16)
    grads2 = [spread(context_grad[at]) for at in spots]
    for n, at in enumerate(spots):
        right_ref[2, at[0], at[1]] = dot(half[n], grads2[n], 0, 0).astype(bf16)
    probs_grad = [dot(g, v, 1, 1) for g, v in zip(grads2, vals1)]
    score_grad = []
    for p, g in zip(probs, probs_grad):
        inner = jnp.sum(g * p, -1, keepdims=True)
        score_grad.append((p * (g - inner) * head_scale).astype(bf16))
    for n, at in enumerate(spots):
        right_ref[0, at[0], at[1]] = gather(dot(score_grad[n], keys1[n])).astype(bf16)
        right_ref[1, at[0], at[1]] = dot(score_grad[n], queries2[n], 0, 0).astype(bf16)
    for m in order[1:]:
        loads["r", m].wait()
    each_block(order[1:], track)

    def sum_copy(k):
        return pltpu.make_async_remote_copy(
            totals.at[k], totals_in.at[k], sum_send.at[k], sum_recv.at[k], (partners[k],), MESH
        )

    def sum_finish(k):
        sum_copy(k).wait()
        totals[k + 1] = totals[k] + totals_in[k]

    own_total = jnp.sum(jnp.sum(squares[...], 0, keepdims=True), 1, keepdims=True)
    totals[0] = jnp.broadcast_to(own_total, totals.shape[1:])
    sum_copy(0).start()

    def mix(m, part, c):
        track_copy(c).wait_recv()
        tracker = 0.5 * (tracked[c].astype(f32) + tracked_in[c].astype(f32))
        own = weights_ref[m, part].astype(f32)
        sent[c] = (own - step_rate * tracker).astype(bf16)
        sent_copy(c).start()
        new_residue_ref[0, m, part] = (tracker - gradient[c]).astype(bf16)
        gradient[c] = 0.5 * own - 0.5 * step_rate * tracker

    def finish(m, part, c):
        sent_copy(c).wait_recv()
        new_weights_ref[0, m, part] = (gradient[c] + 0.5 * sent_in[c].astype(f32)).astype(bf16)

    each_block(order, mix)
    sum_finish(0)
    for at, m in enumerate(order):
        steps_here = range(1 + (steps - 1) * at // matrices, 1 + (steps - 1) * (at + 1) // matrices)
        for k in steps_here:
            sum_copy(k).start()
            if k != steps_here[-1]:
                sum_finish(k)
        each_block([m], finish)
        if steps_here:
            sum_finish(steps_here[-1])
    entries = nodes * matrices * width * width
    rms_ref[0] = jnp.max(jnp.sqrt(totals[steps] / entries))

    @pl.loop(0, matrices * per_matrix)
    def _(c):
        track_copy(c).wait_send()
        sent_copy(c).wait_send()


def one_round(nodes, level, sample_ids, token_pool, cotangent_pool, weights, residue):
    pool, seq, width = token_pool.shape[1:]
    matrices = weights.shape[1]
    rows = pool * seq
    chunks = matrices * (width // CHUNK_ROWS)
    steps = nodes.bit_length() - 1
    chunked = (chunks, CHUNK_ROWS, width)
    dma = pltpu.SemaphoreType.DMA
    return pl.pallas_call(
        partial(round_kernel, nodes, 2**level),
        out_shape=(
            jax.ShapeDtypeStruct(weights.shape, bf16),
            jax.ShapeDtypeStruct(weights.shape, bf16),
            jax.ShapeDtypeStruct((1,), f32),
        ),
        in_specs=[SMEM] + [HBM] * 4,
        out_specs=(VMEM, VMEM, SMEM),
        scratch_shapes=[
            pltpu.VMEM((pool, seq, width), bf16),
            pltpu.VMEM((pool, seq, width), bf16),
            pltpu.VMEM(weights.shape[1:], bf16),
            pltpu.VMEM(weights.shape[1:], bf16),
            pltpu.VMEM((2, width, rows), bf16),
            pltpu.VMEM((3, rows, width), bf16),
            pltpu.VMEM((rows, width), f32),
            pltpu.VMEM(chunked, f32),
            pltpu.VMEM(chunked, bf16),
            pltpu.VMEM(chunked, bf16),
            pltpu.VMEM(chunked, bf16),
            pltpu.VMEM(chunked, bf16),
            pltpu.VMEM((8, width), f32),
            pltpu.VMEM((steps + 1, 8, LANES), f32),
            pltpu.VMEM((steps, 8, LANES), f32),
            dma((2 + 2 * matrices,)),
            dma((chunks,)),
            dma((chunks,)),
            dma((chunks,)),
            dma((chunks,)),
            dma((steps,)),
            dma((steps,)),
        ],
        compiler_params=pltpu.CompilerParams(
            collective_id=level, has_side_effects=True, vmem_limit_bytes=40 * 2**20
        ),
    )(sample_ids, token_pool, cotangent_pool, weights, residue)


def per_device(round_index, sample_ids, token_pool, cotangent_pool, weights, residue):
    nodes = lax.axis_size("node")
    levels = nodes.bit_length() - 1
    new_weights, new_residue, grad_rms = lax.switch(
        round_index[0] % levels,
        [partial(one_round, nodes, level) for level in range(levels)],
        sample_ids,
        token_pool,
        cotangent_pool,
        weights,
        residue,
    )
    return (new_weights, new_residue, grad_rms[0])


def solution(mesh):
    placed = (
        P(),
        P("node", None),
        P("node", None, None, None),
        P("node", None, None, None),
        P("node", None, None, None),
        P("node", None, None, None),
    )
    return jax.shard_map(
        per_device,
        mesh=mesh,
        in_specs=placed,
        out_specs=(P("node", None, None, None), P("node", None, None, None), P()),
        check_vma=False,
    )
```

```python
from functools import partial

import jax
import jax.numpy as jnp
from jax import lax
from jax.experimental import pallas as pl
from jax.experimental.pallas import tpu as pltpu
from jax.sharding import PartitionSpec as P

HEAD_DIM = 64
LANES = 128
CHUNK_ROWS = 128

epsilon = 1e-06
step_rate = 0.1

f32, bf16 = jnp.float32, jnp.bfloat16
MESH = pl.DeviceIdType.MESH
VMEM = pl.BlockSpec(memory_space=pltpu.VMEM)
SMEM = pl.BlockSpec(memory_space=pltpu.SMEM)
HBM = pl.BlockSpec(memory_space=pl.ANY)


def dot(left, right, left_dim=1, right_dim=0):
    return lax.dot_general(
        left, right, (((left_dim,), (right_dim,)), ((), ())), preferred_element_type=f32
    )


def round_kernel(
    nodes,
    offset,
    ids_ref,
    tokens_hbm,
    cot_hbm,
    weights_hbm,
    residue_hbm,
    new_weights_ref,
    new_residue_ref,
    rms_ref,
    tokens_ref,
    cot_ref,
    weights_ref,
    residue_ref,
    left_ref,
    right_ref,
    context_ref,
    gradient,
    tracked,
    tracked_in,
    sent,
    sent_in,
    squares,
    totals,
    totals_in,
    load_sems,
    track_send,
    track_recv,
    sent_send,
    sent_recv,
    sum_send,
    sum_recv,
):
    me = lax.axis_index("node")
    target = lax.rem(me + offset, nodes)
    source = lax.rem(me + nodes - offset, nodes)
    steps = nodes.bit_length() - 1
    mutual = 2 * offset == nodes
    strides = [2**k for k in range(steps)]
    if not mutual:
        strides = [offset] + [stride for stride in strides if stride != offset]
    partners = [me + stride * (1 - 2 * ((me // stride) % 2)) for stride in strides]

    barrier = pltpu.get_barrier_semaphore()
    for other in [target, source] + partners:
        pl.semaphore_signal(barrier, inc=1, device_id=(other,), device_id_type=MESH)

    pool, seq, width = tokens_ref.shape
    matrices = weights_ref.shape[0]
    batch = ids_ref.shape[1]
    rows = pool * seq
    pairs = width // LANES
    per_matrix = width // CHUNK_ROWS
    proj_scale = width**-0.5
    head_scale = HEAD_DIM**-0.5
    order = [3, 2, 0, 1]

    moves = {"tokens": (tokens_hbm.at[0], tokens_ref), "cot": (cot_hbm.at[0], cot_ref)}
    for m in range(matrices):
        moves["w", m] = (weights_hbm.at[0, m], weights_ref.at[m])
        moves["r", m] = (residue_hbm.at[0, m], residue_ref.at[m])
    when = ["tokens", ("w", 0), ("w", 1), ("w", 2), "cot", ("r", 3), ("w", 3), ("r", 2), ("r", 0), ("r", 1)]
    loads = {name: pltpu.make_async_copy(*moves[name], load_sems.at[n]) for n, name in enumerate(when)}
    for name in when:
        loads[name].start()

    def track_copy(c):
        return pltpu.make_async_remote_copy(
            tracked.at[c], tracked_in.at[c], track_send.at[c], track_recv.at[c], (target,), MESH
        )

    def sent_copy(c):
        return pltpu.make_async_remote_copy(
            sent.at[c], sent_in.at[c], sent_send.at[c], sent_recv.at[c], (target,), MESH
        )

    def weights_copy(m, part, c):
        return pltpu.make_async_remote_copy(
            weights_hbm.at[0, m, part],
            sent_in.at[c],
            sent_send.at[c],
            sent_recv.at[c],
            (target,),
            MESH,
        )

    def each_block(which, body):
        for m in which:

            @pl.loop(0, per_matrix)
            def _(r):
                body(m, pl.ds(r * CHUNK_ROWS, CHUNK_ROWS), order.index(m) * per_matrix + r)

    def send_weights(m, part, c):
        weights_copy(m, part, c).start()

    if mutual:
        pl.semaphore_wait(barrier, 2 + steps)
        each_block(order[:2], send_weights)

    counts = []
    for image in range(pool):
        count = jnp.int32(0)
        for draw in range(batch):
            count = count + (ids_ref[0, draw] == image).astype(jnp.int32)
        counts.append(count.astype(f32))

    loads["tokens"].wait()
    values = tokens_ref[...].reshape(rows, width).astype(f32)
    centered = values - jnp.mean(values, -1, keepdims=True)
    variance = jnp.mean(centered * centered, -1, keepdims=True)
    unit_rows = centered * lax.rsqrt(variance + epsilon)
    normed = unit_rows.astype(bf16)
    first = lax.broadcasted_iota(jnp.int32, (seq, LANES), 1) < HEAD_DIM
    units = [(i, j) for i in range(pool) for j in range(pairs)]
    spots = [
        (slice(i * seq, (i + 1) * seq), slice(j * LANES, (j + 1) * LANES)) for i, j in units
    ]

    def spread(block):
        zero = jnp.zeros_like(block)
        return jnp.concatenate([jnp.where(first, block, zero), jnp.where(first, zero, block)], 0)

    def gather(block):
        return jnp.where(first, block[:seq], block[seq:])

    def track(m, part, c):
        right = right_ref[m] if m < 3 else cot_ref[...].reshape(rows, width)
        grad = dot(left_ref[m // 3, part], right) * proj_scale
        gradient[c] = grad
        tracked[c] = (residue_ref[m, part].astype(f32) + grad).astype(bf16)
        track_copy(c).start()
        squares[...] += jnp.sum((grad * grad).reshape(-1, 8, width), 0)

    squares[...] = jnp.zeros_like(squares)
    for m in range(3):
        loads["w", m].wait()
    loads["cot"].wait()
    loads["r", 3].wait()
    queries2, keys1, vals1, probs, half = {}, {}, {}, {}, {}
    for j in range(pairs):
        cols = slice(j * LANES, (j + 1) * LANES)
        queries, keys, vals = [
            (dot(normed, weights_ref[m, :, cols]) * proj_scale).astype(bf16) for m in range(3)
        ]
        here = [(i, j) for i in range(pool)]
        for i, u in enumerate(here):
            part = slice(i * seq, (i + 1) * seq)
            queries2[u], keys1[u], vals1[u] = spread(queries[part]), keys[part], vals[part]
        scores = [dot(queries2[u], keys1[u], 1, 1) * head_scale for u in here]
        for u, score in zip(here, scores):
            e = jnp.exp(score - jnp.max(score, -1, keepdims=True))
            probs[u] = e / jnp.sum(e, -1, keepdims=True)
            half[u] = probs[u].astype(bf16)
        context = [gather(dot(half[u], vals1[u])) * counts[u[0]] for u in here]
        left_ref[1, cols] = jnp.concatenate(context, 0).T.astype(bf16)
        if j == 0 and not mutual:
            pl.semaphore_wait(barrier, 2 + steps)
        track(3, pl.ds(j * LANES, LANES), order.index(3) * per_matrix + j)

    loads["w", 3].wait()
    cot = cot_ref[...].reshape(rows, width)
    context_grad = (dot(cot, weights_ref[3], 1, 1) * proj_scale).astype(bf16)
    weighted = [unit_rows[i * seq : (i + 1) * seq] * counts[i] for i in range(pool)]
    left_ref[0] = jnp.concatenate(weighted, 0).T.astype(bf16)
    queries2, keys1, vals1, probs, half = [
        [found[u] for u in units] for found in (queries2, keys1, vals1, probs, half)
    ]
    grads2 = [spread(context_grad[at]) for at in spots]
    for n, at in enumerate(spots):
        right_ref[2, at[0], at[1]] = dot(half[n], grads2[n], 0, 0).astype(bf16)
    probs_grad = [dot(g, v, 1, 1) for g, v in zip(grads2, vals1)]
    score_grad = []
    for p, g in zip(probs, probs_grad):
        inner = jnp.sum(g * p, -1, keepdims=True)
        score_grad.append((p * (g - inner) * head_scale).astype(bf16))
    for n, at in enumerate(spots):
        right_ref[0, at[0], at[1]] = gather(dot(score_grad[n], keys1[n])).astype(bf16)
        right_ref[1, at[0], at[1]] = dot(score_grad[n], queries2[n], 0, 0).astype(bf16)
    for m in order[1:]:
        loads["r", m].wait()
    each_block(order[1:], track)

    def sum_copy(k):
        return pltpu.make_async_remote_copy(
            totals.at[k], totals_in.at[k], sum_send.at[k], sum_recv.at[k], (partners[k],), MESH
        )

    def sum_finish(k):
        sum_copy(k).wait()
        totals[k + 1] = totals[k] + totals_in[k]

    own_total = jnp.sum(jnp.sum(squares[...], 0, keepdims=True), 1, keepdims=True)
    totals[0] = jnp.broadcast_to(own_total, totals.shape[1:])
    entries = nodes * matrices * width * width

    def set_rms():
        rms_ref[0] = jnp.max(jnp.sqrt(totals[steps] / entries))

    def mix(m, part, c):
        track_copy(c).wait_recv()
        tracker = 0.5 * (tracked[c].astype(f32) + tracked_in[c].astype(f32))
        own = weights_ref[m, part].astype(f32)
        new_residue_ref[0, m, part] = (tracker - gradient[c]).astype(bf16)
        base = 0.5 * own - 0.5 * step_rate * tracker
        if mutual:
            weights_copy(m, part, c).wait_recv()
            peer_sent = (sent_in[c].astype(f32) - step_rate * tracker).astype(bf16)
            new_weights_ref[0, m, part] = (base + 0.5 * peer_sent.astype(f32)).astype(bf16)
        else:
            sent[c] = (own - step_rate * tracker).astype(bf16)
            sent_copy(c).start()
            gradient[c] = base

    def finish(m, part, c):
        sent_copy(c).wait_recv()
        new_weights_ref[0, m, part] = (gradient[c] + 0.5 * sent_in[c].astype(f32)).astype(bf16)

    def drain(m, part, c):
        track_copy(c).wait_send()
        (weights_copy(m, part, c) if mutual else sent_copy(c)).wait_send()

    if mutual:
        for k in range(steps - 2):
            sum_copy(k).start()
            sum_finish(k)
        for n, k in enumerate([steps - 2, steps - 1]):
            sum_copy(k).start()
            each_block([order[2 + n]], send_weights)
            each_block([order[n]], mix)
            sum_finish(k)
        set_rms()
        each_block(order[2:], mix)
    else:
        sum_copy(0).start()
        each_block(order, mix)
        sum_finish(0)
        spans = len(order) - 1
        for at, m in enumerate(order[:-1]):
            here = range(1 + (steps - 1) * at // spans, 1 + (steps - 1) * (at + 1) // spans)
            for k in here:
                sum_copy(k).start()
                if k != here[-1]:
                    sum_finish(k)
            each_block([m], finish)
            if here:
                sum_finish(here[-1])
        set_rms()
        each_block(order[-1:], finish)
    each_block(order, drain)


def one_round(nodes, level, sample_ids, token_pool, cotangent_pool, weights, residue):
    pool, seq, width = token_pool.shape[1:]
    matrices = weights.shape[1]
    rows = pool * seq
    chunks = matrices * (width // CHUNK_ROWS)
    steps = nodes.bit_length() - 1
    chunked = (chunks, CHUNK_ROWS, width)
    dma = pltpu.SemaphoreType.DMA
    return pl.pallas_call(
        partial(round_kernel, nodes, 2**level),
        out_shape=(
            jax.ShapeDtypeStruct(weights.shape, bf16),
            jax.ShapeDtypeStruct(weights.shape, bf16),
            jax.ShapeDtypeStruct((1,), f32),
        ),
        in_specs=[SMEM] + [HBM] * 4,
        out_specs=(VMEM, VMEM, SMEM),
        scratch_shapes=[
            pltpu.VMEM((pool, seq, width), bf16),
            pltpu.VMEM((pool, seq, width), bf16),
            pltpu.VMEM(weights.shape[1:], bf16),
            pltpu.VMEM(weights.shape[1:], bf16),
            pltpu.VMEM((2, width, rows), bf16),
            pltpu.VMEM((3, rows, width), bf16),
            pltpu.VMEM((rows, width), f32),
            pltpu.VMEM(chunked, f32),
            pltpu.VMEM(chunked, bf16),
            pltpu.VMEM(chunked, bf16),
            pltpu.VMEM(chunked, bf16),
            pltpu.VMEM(chunked, bf16),
            pltpu.VMEM((8, width), f32),
            pltpu.VMEM((steps + 1, 8, LANES), f32),
            pltpu.VMEM((steps, 8, LANES), f32),
            dma((2 + 2 * matrices,)),
            dma((chunks,)),
            dma((chunks,)),
            dma((chunks,)),
            dma((chunks,)),
            dma((steps,)),
            dma((steps,)),
        ],
        compiler_params=pltpu.CompilerParams(
            collective_id=level, has_side_effects=True, vmem_limit_bytes=40 * 2**20
        ),
    )(sample_ids, token_pool, cotangent_pool, weights, residue)


def write_kernel(weights_ref, residue_ref, weights_out, residue_out, sems):
    copies = []
    for n, (src, dst) in enumerate([(weights_ref, weights_out), (residue_ref, residue_out)]):
        for m in range(src.shape[1]):
            copies.append(pltpu.make_async_copy(src.at[0, m], dst.at[0, m], sems.at[n, m]))
    for copy in copies:
        copy.start()
    for copy in copies:
        copy.wait()


def write_out(new_weights, new_residue):
    shape = jax.ShapeDtypeStruct(new_weights.shape, bf16)
    return pl.pallas_call(
        write_kernel,
        out_shape=(shape, shape),
        in_specs=[VMEM, VMEM],
        out_specs=(HBM, HBM),
        scratch_shapes=[pltpu.SemaphoreType.DMA((2, new_weights.shape[1]))],
        compiler_params=pltpu.CompilerParams(vmem_limit_bytes=8 * 2**20),
    )(new_weights, new_residue)


def per_device(round_index, sample_ids, token_pool, cotangent_pool, weights, residue):
    nodes = lax.axis_size("node")
    levels = nodes.bit_length() - 1
    new_weights, new_residue, grad_rms = lax.switch(
        round_index[0] % levels,
        [partial(one_round, nodes, level) for level in range(levels)],
        sample_ids,
        token_pool,
        cotangent_pool,
        weights,
        residue,
    )
    new_weights, new_residue = write_out(new_weights, new_residue)
    return (new_weights, new_residue, grad_rms[0])


def solution(mesh):
    placed = (
        P(),
        P("node", None),
        P("node", None, None, None),
        P("node", None, None, None),
        P("node", None, None, None),
        P("node", None, None, None),
    )
    return jax.shard_map(
        per_device,
        mesh=mesh,
        in_specs=placed,
        out_specs=(P("node", None, None, None), P("node", None, None, None), P()),
        check_vma=False,
    )
```
